64 devices in a mesh: rep: 8 (over x, y, core), dp: 8 (over z).
Axes of the slice: x: 2, y: 2, z: 8, core: 2. Of those that a mesh axis runs over, the one named last changes fastest.
The devices are a block of a 4x4x8 slice.
Arguments:
- x: bfloat16 [64, 2048, 640], P(('rep', 'dp')), parts along dimension 0
- dy: bfloat16 [64, 2048, 640], P(('rep', 'dp')), parts along dimension 0
- w_gate: bfloat16 [2, 640, 1792], P(None, 'dp')
- w_up: bfloat16 [2, 640, 1792], P(None, 'dp')
- w_down: bfloat16 [2, 1792, 640], P(None, 'dp')
- m_w_gate: float32 [2, 640, 1792], P(None, 'dp')
- m_w_up: float32 [2, 640, 1792], P(None, 'dp')
- m_w_down: float32 [2, 1792, 640], P(None, 'dp')
- v_w_gate: float32 [2, 640, 1792], P(None, 'dp')
- v_w_up: float32 [2, 640, 1792], P(None, 'dp')
- v_w_down: float32 [2, 1792, 640], P(None, 'dp')
Outputs:
- output 1: bfloat16 [16, 640, 1792], P('rep', 'dp'), parts along dimension 0
- output 2: bfloat16 [16, 640, 1792], P('rep', 'dp'), parts along dimension 0
- output 3: bfloat16 [16, 1792, 640], P('rep', 'dp'), parts along dimension 0
- output 4: float32 [16, 640, 1792], P('rep', 'dp'), parts along dimension 0
- output 5: float32 [16, 640, 1792], P('rep', 'dp'), parts along dimension 0
- output 6: float32 [16, 1792, 640], P('rep', 'dp'), parts along dimension 0
- output 7: float32 [16, 640, 1792], P('rep', 'dp'), parts along dimension 0
- output 8: float32 [16, 640, 1792], P('rep', 'dp'), parts along dimension 0
- output 9: float32 [16, 1792, 640], P('rep', 'dp'), parts along dimension 0
There are 8 independent parts. The reference program is written for one: setup_inputs(seed, part) draws one part's arguments, and reference() takes and returns one part's arrays. A program takes and returns all parts, laid end to end along the dimension named above; an argument that names none is the same for every part.
All inputs are finite; a program needn't handle non-finite values.
Results may differ from the reference program's by a relative error of at most 0.022.
Values are sent between devices in bfloat16 or wider.
A program may use at most 768 MiB of HBM per device.

```python
import jax
import jax.numpy as jnp
from jax import lax

SEQUENCES = 8
TOKENS = 2048
D = 640
FF = 1792
LAYERS = 2
NAMES = ("w_gate", "w_up", "w_down")
SHAPES = {"w_gate": (LAYERS, D, FF), "w_up": (LAYERS, D, FF), "w_down": (LAYERS, FF, D)}


def bump(key, n, height):
    away = (jnp.arange(n, dtype=jnp.int32) - jax.random.randint(key, (), 0, n, jnp.int32)) % n
    return jnp.where(away < n // 8, height, 1.0)


def together(key, own, strength):
    shared = jax.random.normal(key, own.shape[1:], jnp.float32)
    return (own + strength * shared) * lax.rsqrt(1 + strength * strength)


def setup_inputs(seed: int = 0, part: int = 0) -> dict:
    kx, kdy, ka, kb, kz, kf, kh, kl, *keys = jax.random.split(jax.random.key(seed), 8 + 3 * len(NAMES))
    kx, kdy, ka, kb = (jax.random.fold_in(k, part) for k in (kx, kdy, ka, kb))
    kw, km, kv = (keys[i::3] for i in range(3))
    shape = (SEQUENCES, TOKENS, D)
    much_x, much_dy = jax.random.uniform(kz, (2,), jnp.float32, 0.0, 1.0)
    loud = 2.0 ** jax.random.uniform(jax.random.fold_in(kz, 1), (), jnp.float32, -1.0, 2.0)
    layers = 2.0 ** jax.random.uniform(kl, (LAYERS, 1, 1), jnp.float32, -1.0, 1.0)
    x = together(ka, jax.random.normal(kx, shape, jnp.float32), much_x) * bump(kf, D, 4.0)
    dy = together(kb, jax.random.normal(kdy, shape, jnp.float32), much_dy)
    drawn = {"x": x.astype(jnp.bfloat16), "dy": (loud * dy * (SEQUENCES * TOKENS) ** -0.5).astype(jnp.bfloat16)}
    for key, name in zip(kw, NAMES, strict=True):
        w = jax.random.normal(key, SHAPES[name], jnp.float32) * SHAPES[name][1] ** -0.5
        drawn[name] = (w * {"w_gate": 1.0, "w_up": bump(kh, FF, 4.0), "w_down": layers}[name]).astype(jnp.bfloat16)
    for key, name in zip(km, NAMES, strict=True):
        drawn[f"m_{name}"] = 0.1 * jax.random.normal(key, SHAPES[name], jnp.float32)
    for key, name in zip(kv, NAMES, strict=True):
        drawn[f"v_{name}"] = jax.random.uniform(key, SHAPES[name], jnp.float32, 0.005, 0.015)
    return drawn


def matmul(a, w):
    return jnp.dot(a, w, preferred_element_type=jnp.float32).astype(jnp.bfloat16)


def normed(h):
    wide = h.astype(jnp.float32)
    scale = lax.rsqrt(jnp.mean(wide**2, -1, keepdims=True) + 1e-6)
    return (wide * scale).astype(jnp.bfloat16)


def layer(h, w):
    a = normed(h)
    gate = jnp.dot(a, w["w_gate"], preferred_element_type=jnp.float32)
    up = jnp.dot(a, w["w_up"], preferred_element_type=jnp.float32)
    return h + matmul((jax.nn.silu(gate) * up).astype(jnp.bfloat16), w["w_down"])


def adamw(w, m, v, g):
    m = 0.9 * m + 0.1 * g
    v = 0.95 * v + 0.05 * g * g
    step = m * lax.rsqrt(v + 1e-8) + 0.1 * w
    return (w - 0.02 * step).astype(jnp.bfloat16), m, v


def clipped(gradients, sum_of_squares, count):
    factor = jnp.minimum(1.0, 0.5 * lax.rsqrt(sum_of_squares / count + 1e-30))
    return [g * factor for g in gradients]


def stack(weights, h):
    return lax.scan(lambda h, w: (layer(h, w), None), h, weights)[0]


def reference(x, dy, w_gate, w_up, w_down, m_w_gate, m_w_up, m_w_down, v_w_gate, v_w_up, v_w_down):
    weights = dict(zip(NAMES, (w_gate, w_up, w_down), strict=True))

    def take(so_far, sequence):
        h, by_y = sequence
        _, back = jax.vjp(lambda w: stack(w, h), weights)
        return jax.tree.map(lambda total, term: total + term.astype(jnp.float32), so_far, back(by_y)[0]), None

    none_yet = {name: jnp.zeros(w.shape, jnp.float32) for name, w in weights.items()}
    by_weights, _ = lax.scan(take, none_yet, (x, dy))
    gradients = [by_weights[name].astype(jnp.bfloat16).astype(jnp.float32) for name in NAMES]
    gradients = clipped(gradients, sum(jnp.sum(g * g) for g in gradients), sum(g.size for g in gradients))
    new = [
        adamw(w.astype(jnp.float32), m, v, g)
        for w, m, v, g in zip((w_gate, w_up, w_down), (m_w_gate, m_w_up, m_w_down), (v_w_gate, v_w_up, v_w_down), gradients, strict=True)
    ]
    return tuple(one[which] for which in range(3) for one in new)
```

```python
import functools

import jax
import jax.numpy as jnp
from jax import lax
from jax.experimental import pallas as pl
from jax.experimental.pallas import tpu as pltpu
from jax.sharding import PartitionSpec as P

F32, BF16 = jnp.float32, jnp.bfloat16
MESH = pl.DeviceIdType.MESH
CHUNK = 256
TILE = 512
SMALL = 256


def dot(a, b):
    return jnp.dot(a, b, preferred_element_type=F32)


def dot_t(a, b):
    return lax.dot_general(a, b, (((1,), (1,)), ((), ())), preferred_element_type=F32)


def scale_of(wide):
    return lax.rsqrt(jnp.mean(wide * wide, -1, keepdims=True) + 1e-6)


def kernel(n, dims, x_hbm, dy_hbm, wg_hbm, wu_hbm, wd_hbm, gg_hbm, gu_hbm, gd_hbm, total_ref,
           wgu, wd, dgu, dd, h, dy, a, at, dyt, acc, hid, dgdu, gu_slot, dn_slot, squares, mine,
           load_sem, out_sem, zrecv, zsend, drecv, dsend, gu_recv, gu_send, dn_recv, dn_send, sq_recv, sq_send):
    tokens, d, ff, rows, down = dims
    half = down // 2
    chunks = ff // CHUNK
    me = lax.axis_index("dp")
    rep = lax.axis_index("rep")
    core = lax.rem(rep, 2)
    partner = rep + 1 - 2 * core
    ahead = (lax.rem(me + 1, n), lax.rem(me + n - 1, n))

    def to(direction):
        return {"dp": ahead[direction]}

    loads = []
    for layer in range(2):
        for which, src in enumerate((wg_hbm, wu_hbm)):
            dst = wgu.at[layer, which, pl.ds(pl.multiple_of(me * rows, 16), rows), :]
            loads.append(pltpu.make_async_copy(src.at[layer], dst, load_sem.at[len(loads)]))
        dst = wd.at[layer, pl.ds(pl.multiple_of(me * down, 16), down), :]
        loads.append(pltpu.make_async_copy(wd_hbm.at[layer], dst, load_sem.at[len(loads)]))
    loads.append(pltpu.make_async_copy(x_hbm.at[0], h, load_sem.at[6]))
    loads.append(pltpu.make_async_copy(dy_hbm.at[0], dy, load_sem.at[7]))
    for one in loads:
        one.start()
    barrier = pltpu.get_barrier_semaphore()
    for k in range(1, n):
        pl.semaphore_signal(barrier, inc=1, device_id={"dp": lax.rem(me + k, n)}, device_id_type=MESH)
    pl.semaphore_signal(barrier, inc=1, device_id={"rep": partner}, device_id_type=MESH)
    pl.semaphore_wait(barrier, n)
    for one in loads:
        one.wait()

    def piece(layer, which, number, direction, block):
        if number < 2:
            wide = ff // 2
            cut = (wide // 128 + 1) // 2 * 128
            off, size = (0, cut) if number == 0 else (cut, wide - cut)
            return wgu.at[layer, which, pl.ds(pl.multiple_of(block * rows, 16), rows), pl.ds(direction * wide + off, size)]
        cut = (half // 16 + 1 - layer) // 2 * 16
        off, size = (0, cut) if direction == 0 else (cut, half - cut)
        return wd.at[layer, pl.ds(pl.multiple_of(block * down + which * half + off, 16), size), :]

    def held(direction, t):
        return lax.rem(me - t + n, n) if direction == 0 else lax.rem(me + t, n)

    def along(layer, number, direction, t):
        ref = piece(layer, core, number, direction, held(direction, t))
        slot = lax.rem(t, 2)
        return pltpu.make_async_remote_copy(ref, ref, zsend.at[layer, number, direction, slot], zrecv.at[layer, number, direction, slot],
                                            device_id=to(direction), device_id_type=MESH)

    def across(layer, which, number, direction, t):
        ref = piece(layer, which, number, direction, held(direction, t))
        slot = lax.rem(t, 2)
        return pltpu.make_async_remote_copy(ref, ref, dsend.at[layer, number, direction, slot], drecv.at[layer, number, direction, slot],
                                            device_id={"rep": partner}, device_id_type=MESH)

    def arrived(layer, number, direction, t):
        ref = piece(layer, core, number, direction, held(direction, t))
        slot = lax.rem(t + 1, 2)
        return pltpu.make_async_remote_copy(ref, ref, zsend.at[layer, number, direction, slot], zrecv.at[layer, number, direction, slot],
                                            device_id=to(direction), device_id_type=MESH)

    def gather_round(layer, t):
        for number in range(3):
            for direction in range(2):
                @pl.when(t >= 1)
                def _():
                    arrived(layer, number, direction, t).wait_recv()

                @pl.when((t >= 2) & (t < n))
                def _():
                    across(layer, 1 - core, number, direction, t - 1).wait_recv()

            for direction in range(2):
                @pl.when((t >= 2) & (t <= n - 2))
                def _():
                    along(layer, number, direction, t - 2).wait_send()

                @pl.when(t <= n - 2)
                def _():
                    along(layer, number, direction, t).start()

                @pl.when(t >= 3)
                def _():
                    across(layer, core, number, direction, t - 2).wait_send()

                @pl.when(t >= 1)
                def _():
                    across(layer, core, number, direction, t).start()

    def gather_end(layer):
        for number in range(3):
            for direction in range(2):
                across(layer, 1 - core, number, direction, n - 1).wait_recv()
                for t in (n - 3, n - 2):
                    along(layer, number, direction, t).wait_send()
                for t in (n - 2, n - 1):
                    across(layer, core, number, direction, t).wait_send()

    def small(k):
        return pl.ds(pl.multiple_of(k * SMALL, SMALL), SMALL)

    steps = tokens // SMALL

    def first(t, _):
        gather_round(0, t)

        @pl.when(t < steps)
        def _():
            wide = h[small(t), :].astype(F32)
            a[0, small(t), :] = (wide * scale_of(wide)).astype(BF16)
            dyt[:, small(t)] = dy[small(t), :].T
        return 0

    lax.fori_loop(0, max(n, steps), first, 0)
    gather_end(0)

    def cols(c):
        return pl.ds(pl.multiple_of(c * CHUNK, CHUNK), CHUNK)

    def forward(c, _):
        gather_round(1, c)

        def tile(k, _):
            r = pl.ds(pl.multiple_of(k * TILE, TILE), TILE)
            gate = dot(a[0, r, :], wgu[0, 0, :, cols(c)])
            up = dot(a[0, r, :], wgu[0, 1, :, cols(c)])
            hidden = (gate * jax.nn.sigmoid(gate) * up).astype(BF16)
            out = dot(hidden, wd[0, cols(c), :])

            @pl.when(c == 0)
            def _():
                acc[r, :] = out

            @pl.when(c > 0)
            def _():
                acc[r, :] += out
            return 0

        lax.fori_loop(0, tokens // TILE, tile, 0)
        return 0

    lax.fori_loop(0, chunks, forward, 0)
    for t in range(chunks, n):
        gather_round(1, t)

    def between(k, _):
        r = small(k)
        h1 = (h[r, :].astype(F32) + acc[r, :].astype(BF16).astype(F32)).astype(BF16)
        h[r, :] = h1
        wide = h1.astype(F32)
        a1 = (wide * scale_of(wide)).astype(BF16)
        a[1, r, :] = a1
        at[:, r] = a1.T
        return 0

    lax.fori_loop(0, steps, between, 0)
    gather_end(1)

    slabs = 2 * chunks

    def block_at(direction, t):
        return lax.rem(me - 1 - t + 2 * n, n) if direction == 0 else lax.rem(me + 1 + t, n)

    def gu_ref(j, direction, t):
        layer = 1 - j // chunks
        r = pl.ds(pl.multiple_of(block_at(direction, t) * rows, 16), rows)
        return dgu.at[layer, direction, r, cols(lax.rem(j, chunks))]

    def gu_copy(r, direction, t):
        slot = lax.rem(r, 2)
        return pltpu.make_async_remote_copy(gu_ref(r - t, direction, t), gu_slot.at[direction, slot, t], gu_send.at[direction, t],
                                            gu_recv.at[direction, slot, t], device_id=to(direction), device_id_type=MESH)

    def gu_round(r):
        def tick(k, _):
            t = n - 1 - k
            j = r - t

            @pl.when((j >= 0) & (j < slabs))
            def _():
                @pl.when(t >= 1)
                def _():
                    for direction in range(2):
                        gu_copy(r - 1, direction, t - 1).wait_recv()
                        mine_ref = gu_ref(j, direction, t)
                        got = gu_slot[direction, lax.rem(r + 1, 2), t - 1].astype(F32)
                        mine_ref[...] = (got + mine_ref[...].astype(F32)).astype(BF16)

            @pl.when((t <= n - 2) & (j >= 1) & (j <= slabs))
            def _():
                for direction in range(2):
                    gu_copy(r - 1, direction, t).wait_send()

            @pl.when((j >= 0) & (j < slabs) & (t <= n - 2))
            def _():
                for direction in range(2):
                    gu_copy(r, direction, t).start()
            return 0

        lax.fori_loop(0, n, tick, 0)

    parts = d // 128

    def dn_ref(layer, s, direction, t):
        r = pl.ds(pl.multiple_of(block_at(direction, t) * down + direction * half, 16), half)
        return dd.at[layer, r, pl.ds(pl.multiple_of(s * 128, 128), 128)]

    def dn_copy(layer, s, direction, t):
        slot = lax.rem(t, 2)
        return pltpu.make_async_remote_copy(dn_ref(layer, s, direction, t), dn_slot.at[layer, direction, slot, s], dn_send.at[layer, direction, s],
                                            dn_recv.at[layer, direction, slot, s], device_id=to(direction), device_id_type=MESH)

    def dn_round(layer, t):
        def part(s, _):
            @pl.when(t >= 1)
            def _():
                for direction in range(2):
                    dn_copy(layer, s, direction, t - 1).wait_recv()
                    mine_ref = dn_ref(layer, s, direction, t)
                    got = dn_slot[layer, direction, lax.rem(t + 1, 2), s].astype(F32)
                    mine_ref[...] = (got + mine_ref[...].astype(F32)).astype(BF16)
                for direction in range(2):
                    dn_copy(layer, s, direction, t - 1).wait_send()

            @pl.when(t <= n - 2)
            def _():
                for direction in range(2):
                    dn_copy(layer, s, direction, t).start()
            return 0

        lax.fori_loop(0, parts, part, 0)

    def backward(layer, c):
        def tile(k, _):
            r = pl.ds(pl.multiple_of(k * TILE, TILE), TILE)
            gate = dot(a[layer, r, :], wgu[layer, 0, :, cols(c)])
            up = dot(a[layer, r, :], wgu[layer, 1, :, cols(c)])
            by = dot_t(dy[r, :], wd[layer, cols(c), :]).astype(BF16).astype(F32)
            sig = jax.nn.sigmoid(gate)
            silu = gate * sig
            hid[r, :] = (silu * up).astype(BF16)
            by_gate = (by * up * (sig + silu * (1.0 - sig))).astype(BF16)
            by_up = (by * silu).astype(BF16)
            dgdu[r, pl.ds(0, CHUNK)] = by_gate
            dgdu[r, pl.ds(CHUNK, CHUNK)] = by_up
            if layer == 1:
                out = dot_t(by_gate, wgu[layer, 0, :, cols(c)]) + dot_t(by_up, wgu[layer, 1, :, cols(c)])

                @pl.when(c == 0)
                def _():
                    acc[r, :] = out

                @pl.when(c > 0)
                def _():
                    acc[r, :] += out
            return 0

        lax.fori_loop(0, tokens // TILE, tile, 0)
        by_w = dot(at[...], dgdu[...])
        dgu[layer, 0, :, cols(c)] = by_w[:, :CHUNK].astype(BF16)
        dgu[layer, 1, :, cols(c)] = by_w[:, CHUNK:].astype(BF16)
        dd[layer, cols(c), :] = dot(dyt[...], hid[...]).T.astype(BF16)

    def last_layer(c, _):
        backward(1, c)
        gu_round(c)
        return 0

    lax.fori_loop(0, chunks, last_layer, 0)

    def norm_back(k, _):
        r = small(k)
        by_a = acc[r, :].astype(BF16).astype(F32)
        wide = h[r, :].astype(F32)
        scale = scale_of(wide)
        by_scale = jnp.sum(by_a * wide, -1, keepdims=True)
        by_wide = by_a * scale - wide * (scale * scale * scale * by_scale * (1.0 / d))
        by_h = (dy[r, :].astype(F32) + by_wide.astype(BF16).astype(F32)).astype(BF16)
        dy[r, :] = by_h
        dyt[:, r] = by_h.T
        at[:, r] = a[0, r, :].T
        return 0

    lax.fori_loop(0, steps, norm_back, 0)

    def first_layer(c, _):
        backward(0, c)
        gu_round(chunks + c)
        dn_round(1, c)
        return 0

    lax.fori_loop(0, chunks, first_layer, 0)
    for t in range(chunks, n):
        dn_round(1, t)

    def drain(k, _):
        gu_round(2 * chunks + k)
        dn_round(0, k)
        return 0

    lax.fori_loop(0, n, drain, 0)

    outs = []
    for layer in range(2):
        for which, dst in enumerate((gg_hbm, gu_hbm)):
            src = dgu.at[layer, which, pl.ds(pl.multiple_of(me * rows, 16), rows), :]
            outs.append(pltpu.make_async_copy(src, dst.at[layer], out_sem.at[len(outs)]))
        src = dd.at[layer, pl.ds(pl.multiple_of(me * down, 16), down), :]
        outs.append(pltpu.make_async_copy(src, gd_hbm.at[layer], out_sem.at[len(outs)]))
    for one in outs:
        one.start()
    sums = jnp.zeros((1, 1), F32)
    for layer in range(2):
        for which in range(2):
            v = dgu[layer, which, pl.ds(pl.multiple_of(me * rows, 16), rows), :].astype(F32)
            sums += jnp.sum(v * v, keepdims=True)
        v = dd[layer, pl.ds(pl.multiple_of(me * down, 16), down), :].astype(F32)
        sums += jnp.sum(v * v, keepdims=True)
    mine[...] = jnp.broadcast_to(sums, mine.shape)

    def spread(k):
        return pltpu.make_async_remote_copy(mine, squares.at[k - 1], sq_send.at[k - 1], sq_recv.at[k - 1],
                                            device_id={"dp": lax.rem(me + k, n)}, device_id_type=MESH)

    for k in range(1, n):
        spread(k).start()
    for k in range(1, n):
        spread(k).wait_recv()
    total = mine[...]
    for k in range(1, n):
        total += squares[k - 1]
    total_ref[...] = total
    for k in range(1, n):
        spread(k).wait_send()
    for one in outs:
        one.wait()


def summed_gradients(n, x, dy, w_gate, w_up, w_down):
    _, tokens, d = x.shape
    layers, rows, ff = w_gate.shape
    down = w_down.shape[1]
    dims = (tokens, d, ff, rows, down)
    half = down // 2
    dma = pltpu.SemaphoreType.DMA
    anywhere = pl.BlockSpec(memory_space=pl.ANY)
    return pl.pallas_call(
        functools.partial(kernel, n, dims),
        out_shape=(
            jax.ShapeDtypeStruct(w_gate.shape, BF16),
            jax.ShapeDtypeStruct(w_up.shape, BF16),
            jax.ShapeDtypeStruct(w_down.shape, BF16),
            jax.ShapeDtypeStruct((8, 128), F32),
        ),
        in_specs=[anywhere] * 5,
        out_specs=(anywhere,) * 3 + (pl.BlockSpec(memory_space=pltpu.VMEM),),
        scratch_shapes=[
            pltpu.VMEM((layers, 2, d, ff), BF16),
            pltpu.VMEM((layers, ff, d), BF16),
            pltpu.VMEM((layers, 2, d, ff), BF16),
            pltpu.VMEM((layers, ff, d), BF16),
            pltpu.VMEM((tokens, d), BF16),
            pltpu.VMEM((tokens, d), BF16),
            pltpu.VMEM((layers, tokens, d), BF16),
            pltpu.VMEM((d, tokens), BF16),
            pltpu.VMEM((d, tokens), BF16),
            pltpu.VMEM((tokens, d), F32),
            pltpu.VMEM((tokens, CHUNK), BF16),
            pltpu.VMEM((tokens, 2 * CHUNK), BF16),
            pltpu.VMEM((2, 2, n - 1, rows, CHUNK), BF16),
            pltpu.VMEM((2, 2, 2, d // 128, half, 128), BF16),
            pltpu.VMEM((n - 1, 8, 128), F32),
            pltpu.VMEM((8, 128), F32),
            dma((8,)),
            dma((6,)),
            dma((2, 3, 2, 2)),
            dma((2, 3, 2, 2)),
            dma((2, 3, 2, 2)),
            dma((2, 3, 2, 2)),
            dma((2, 2, n - 1)),
            dma((2, n - 1)),
            dma((2, 2, 2, d // 128)),
            dma((2, 2, d // 128)),
            dma((n - 1,)),
            dma((n - 1,)),
        ],
        compiler_params=pltpu.CompilerParams(collective_id=0, has_side_effects=True, vmem_limit_bytes=67_000_000),
    )(x, dy, w_gate, w_up, w_down)


def adamw(w, m, v, g):
    m = 0.9 * m + 0.1 * g
    v = 0.95 * v + 0.05 * g * g
    step = m * lax.rsqrt(v + 1e-8) + 0.1 * w
    return (w - 0.02 * step).astype(BF16), m, v


def solution(mesh):
    n = mesh.shape["dp"]

    def step(x, dy, *arrays):
        weights, m, v = (arrays[i : i + 3] for i in (0, 3, 6))
        *gradients, squares = summed_gradients(n, x, dy, *weights)
        count = n * sum(g.size for g in gradients)
        factor = jnp.minimum(1.0, 0.5 * lax.rsqrt(squares[0, 0] / count + 1e-30))
        new = [adamw(w.astype(F32), m, v, g.astype(F32) * factor) for w, m, v, g in zip(weights, m, v, gradients, strict=True)]
        return tuple(one[which] for which in range(3) for one in new)

    states, cut = P(("rep", "dp"), None, None), P(None, "dp", None)
    return jax.shard_map(
        step,
        mesh=mesh,
        in_specs=(states, states) + (cut,) * 9,
        out_specs=(P("rep", "dp", None),) * 9,
        check_vma=False,
    )
```

```python
import functools

import jax
import jax.numpy as jnp
from jax import lax
from jax.experimental import pallas as pl
from jax.experimental.pallas import tpu as pltpu
from jax.sharding import PartitionSpec as P

F32, BF16 = jnp.float32, jnp.bfloat16
MESH = pl.DeviceIdType.MESH
CHUNK = 256
TILE = 512
SMALL = 256


def dot(a, b):
    return jnp.dot(a, b, preferred_element_type=F32)


def dot_t(a, b):
    return lax.dot_general(a, b, (((1,), (1,)), ((), ())), preferred_element_type=F32)


def scale_of(wide):
    return lax.rsqrt(jnp.mean(wide * wide, -1, keepdims=True) + 1e-6)


def kernel(n, dims, x_hbm, dy_hbm, wg_hbm, wu_hbm, wd_hbm, gg_hbm, gu_hbm, gd_hbm, total_ref,
           wgu, wd, dgu, dd, h, dy, a, at, dyt, acc, hid, dgdu, gu_slot, dn_slot, squares, mine,
           load_sem, out_sem, zrecv, zsend, drecv, dsend, gu_recv, gu_send, dn_recv, dn_send, sq_recv, sq_send):
    tokens, d, ff, rows, down = dims
    half = down // 2
    chunks = ff // CHUNK
    me = lax.axis_index("dp")
    rep = lax.axis_index("rep")
    core = lax.rem(rep, 2)
    partner = rep + 1 - 2 * core
    ahead = (lax.rem(me + 1, n), lax.rem(me + n - 1, n))

    def to(direction):
        return {"dp": ahead[direction]}

    loads = []
    for layer in range(2):
        for which, src in enumerate((wg_hbm, wu_hbm)):
            dst = wgu.at[layer, which, pl.ds(pl.multiple_of(me * rows, 16), rows), :]
            loads.append(pltpu.make_async_copy(src.at[layer], dst, load_sem.at[len(loads)]))
        dst = wd.at[layer, pl.ds(pl.multiple_of(me * down, 16), down), :]
        loads.append(pltpu.make_async_copy(wd_hbm.at[layer], dst, load_sem.at[len(loads)]))
    loads.append(pltpu.make_async_copy(x_hbm.at[0], h, load_sem.at[6]))
    loads.append(pltpu.make_async_copy(dy_hbm.at[0], dy, load_sem.at[7]))
    for one in loads:
        one.start()
    barrier = pltpu.get_barrier_semaphore()
    for k in range(1, n):
        pl.semaphore_signal(barrier, inc=1, device_id={"dp": lax.rem(me + k, n)}, device_id_type=MESH)
    pl.semaphore_signal(barrier, inc=1, device_id={"rep": partner}, device_id_type=MESH)
    pl.semaphore_wait(barrier, n)
    for one in loads[:6]:
        one.wait()

    def piece(layer, which, number, direction, block):
        if number < 2:
            wide = ff // 2
            cut = (wide // 128 + 1) // 2 * 128
            off, size = (0, cut) if number == 0 else (cut, wide - cut)
            return wgu.at[layer, which, pl.ds(pl.multiple_of(block * rows, 16), rows), pl.ds(direction * wide + off, size)]
        cut = (half // 16 + 1 - layer) // 2 * 16
        off, size = (0, cut) if direction == 0 else (cut, half - cut)
        return wd.at[layer, pl.ds(pl.multiple_of(block * down + which * half + off, 16), size), :]

    def held(direction, t):
        return lax.rem(me - t + n, n) if direction == 0 else lax.rem(me + t, n)

    def along(layer, number, direction, t):
        ref = piece(layer, core, number, direction, held(direction, t))
        slot = lax.rem(t, 2)
        return pltpu.make_async_remote_copy(ref, ref, zsend.at[layer, number, direction, slot], zrecv.at[layer, number, direction, slot],
                                            device_id=to(direction), device_id_type=MESH)

    def across(layer, which, number, direction, t):
        ref = piece(layer, which, number, direction, held(direction, t))
        slot = lax.rem(t, 2)
        return pltpu.make_async_remote_copy(ref, ref, dsend.at[layer, number, direction, slot], drecv.at[layer, number, direction, slot],
                                            device_id={"rep": partner}, device_id_type=MESH)

    def arrived(layer, number, direction, t):
        ref = piece(layer, core, number, direction, held(direction, t))
        slot = lax.rem(t + 1, 2)
        return pltpu.make_async_remote_copy(ref, ref, zsend.at[layer, number, direction, slot], zrecv.at[layer, number, direction, slot],
                                            device_id=to(direction), device_id_type=MESH)

    def gather_round(layer, t):
        for number in range(3):
            for direction in range(2):
                @pl.when(t >= 1)
                def _():
                    arrived(layer, number, direction, t).wait_recv()

                @pl.when((t >= 2) & (t < n))
                def _():
                    across(layer, 1 - core, number, direction, t - 1).wait_recv()

            for direction in range(2):
                @pl.when((t >= 2) & (t <= n - 2))
                def _():
                    along(layer, number, direction, t - 2).wait_send()

                @pl.when(t <= n - 2)
                def _():
                    along(layer, number, direction, t).start()

                @pl.when(t >= 3)
                def _():
                    across(layer, core, number, direction, t - 2).wait_send()

                @pl.when(t >= 1)
                def _():
                    across(layer, core, number, direction, t).start()

    def gather_end(layer):
        for number in range(3):
            for direction in range(2):
                across(layer, 1 - core, number, direction, n - 1).wait_recv()
                for t in (n - 3, n - 2):
                    along(layer, number, direction, t).wait_send()
                for t in (n - 2, n - 1):
                    across(layer, core, number, direction, t).wait_send()

    def small(k):
        return pl.ds(pl.multiple_of(k * SMALL, SMALL), SMALL)

    steps = tokens // SMALL

    gather_round(0, 0)
    for one in loads[6:]:
        one.wait()

    def first(t, _):
        @pl.when(t >= 1)
        def _():
            gather_round(0, t)

        @pl.when(t < steps)
        def _():
            wide = h[small(t), :].astype(F32)
            a[0, small(t), :] = (wide * scale_of(wide)).astype(BF16)
            dyt[:, small(t)] = dy[small(t), :].T
            acc[small(t), :] = jnp.zeros((SMALL, d), F32)
        return 0

    lax.fori_loop(0, max(n, steps), first, 0)
    gather_end(0)

    def cols(c):
        return pl.ds(pl.multiple_of(c * CHUNK, CHUNK), CHUNK)

    def forward(c, _):
        gather_round(1, c)

        def tile(k, _):
            r = pl.ds(pl.multiple_of(k * TILE, TILE), TILE)
            both = dot(a[0, r, :], jnp.concatenate([wgu[0, 0, :, cols(c)], wgu[0, 1, :, cols(c)]], 1))
            gate, up = both[:, :CHUNK], both[:, CHUNK:]
            hidden = (gate * jax.nn.sigmoid(gate) * up).astype(BF16)
            acc[r, :] += dot(hidden, wd[0, cols(c), :])
            return 0

        lax.fori_loop(0, tokens // TILE, tile, 0)
        return 0

    lax.fori_loop(0, chunks, forward, 0)
    for t in range(chunks, n):
        gather_round(1, t)

    def between(k, _):
        r = small(k)
        h1 = (h[r, :].astype(F32) + acc[r, :].astype(BF16).astype(F32)).astype(BF16)
        h[r, :] = h1
        wide = h1.astype(F32)
        a1 = (wide * scale_of(wide)).astype(BF16)
        a[1, r, :] = a1
        at[:, r] = a1.T
        acc[r, :] = jnp.zeros((SMALL, d), F32)
        return 0

    lax.fori_loop(0, steps, between, 0)
    gather_end(1)

    slabs = 2 * chunks

    def block_at(direction, t):
        return lax.rem(me - 1 - t + 2 * n, n) if direction == 0 else lax.rem(me + 1 + t, n)

    def gu_ref(j, direction, t):
        layer = 1 - j // chunks
        r = pl.ds(pl.multiple_of(block_at(direction, t) * rows, 16), rows)
        return dgu.at[layer, direction, r, cols(lax.rem(j, chunks))]

    def gu_copy(j, direction, t):
        slot = lax.rem(j, 2)
        return pltpu.make_async_remote_copy(gu_ref(j, direction, t), gu_slot.at[direction, slot, t], gu_send.at[direction, slot, t],
                                            gu_recv.at[direction, slot, t], device_id=to(direction), device_id_type=MESH)

    def gu_round(r):
        def tick(k, _):
            i = n // 2 - 1 - k
            t = lax.rem(r, 2) + 2 * i
            j = r // 2 - i

            @pl.when((j >= 0) & (j < slabs))
            def _():
                @pl.when(t >= 1)
                def _():
                    for direction in range(2):
                        gu_copy(j, direction, t - 1).wait_recv()
                        mine_ref = gu_ref(j, direction, t)
                        got = gu_slot[direction, lax.rem(j, 2), t - 1].astype(F32)
                        mine_ref[...] = (got + mine_ref[...].astype(F32)).astype(BF16)
                    for direction in range(2):
                        gu_copy(j, direction, t - 1).wait_send()

                @pl.when(t <= n - 2)
                def _():
                    for direction in range(2):
                        gu_copy(j, direction, t).start()
            return 0

        lax.fori_loop(0, n // 2, tick, 0)

    parts = d // 128

    def dn_ref(layer, s, direction, t):
        r = pl.ds(pl.multiple_of(block_at(direction, t) * down + direction * half, 16), half)
        return dd.at[layer, r, pl.ds(pl.multiple_of(s * 128, 128), 128)]

    def dn_copy(layer, s, direction, t):
        slot = lax.rem(t, 2)
        return pltpu.make_async_remote_copy(dn_ref(layer, s, direction, t), dn_slot.at[layer, direction, slot, s], dn_send.at[layer, direction, s],
                                            dn_recv.at[layer, direction, slot, s], device_id=to(direction), device_id_type=MESH)

    def dn_round(layer, t):
        def part(s, _):
            @pl.when(t >= 1)
            def _():
                for direction in range(2):
                    dn_copy(layer, s, direction, t - 1).wait_recv()
                    mine_ref = dn_ref(layer, s, direction, t)
                    got = dn_slot[layer, direction, lax.rem(t + 1, 2), s].astype(F32)
                    mine_ref[...] = (got + mine_ref[...].astype(F32)).astype(BF16)
                for direction in range(2):
                    dn_copy(layer, s, direction, t - 1).wait_send()

            @pl.when(t <= n - 2)
            def _():
                for direction in range(2):
                    dn_copy(layer, s, direction, t).start()
            return 0

        lax.fori_loop(0, parts, part, 0)

    def backward(layer, c, between_halves):
        def tile(k, _):
            r = pl.ds(pl.multiple_of(k * TILE, TILE), TILE)
            wide = jnp.concatenate([wgu[layer, 0, :, cols(c)], wgu[layer, 1, :, cols(c)]], 1)
            both = dot(a[layer, r, :], wide)
            gate, up = both[:, :CHUNK], both[:, CHUNK:]
            by = dot_t(dy[r, :], wd[layer, cols(c), :]).astype(BF16).astype(F32)
            sig = jax.nn.sigmoid(gate)
            silu = gate * sig
            hid[r, :] = (silu * up).astype(BF16)
            by_gate = (by * up * (sig + silu * (1.0 - sig))).astype(BF16)
            by_up = (by * silu).astype(BF16)
            by_both = jnp.concatenate([by_gate, by_up], 1)
            dgdu[r, :] = by_both
            if layer == 1:
                acc[r, :] += dot_t(by_both, wide)
            return 0

        lax.fori_loop(0, tokens // TILE, tile, 0)
        between_halves()
        by_w = dot(at[...], dgdu[...])
        dgu[layer, 0, :, cols(c)] = by_w[:, :CHUNK].astype(BF16)
        dgu[layer, 1, :, cols(c)] = by_w[:, CHUNK:].astype(BF16)
        dd[layer, cols(c), :] = dot(dyt[...], hid[...]).T.astype(BF16)

    def last_layer(c, _):
        def between_halves():
            @pl.when(c >= 1)
            def _():
                gu_round(2 * c - 1)

        backward(1, c, between_halves)
        gu_round(2 * c)
        return 0

    lax.fori_loop(0, chunks, last_layer, 0)

    early = min(2, steps)

    def norm_back(k, _):
        r = small(k)

        @pl.when(k == 0)
        def _():
            dn_round(1, 0)

        @pl.when(k == steps // 2)
        def _():
            gu_round(2 * chunks - 1)
            dn_round(1, 1)
        by_a = acc[r, :].astype(BF16).astype(F32)
        wide = h[r, :].astype(F32)
        scale = scale_of(wide)
        by_scale = jnp.sum(by_a * wide, -1, keepdims=True)
        by_wide = by_a * scale - wide * (scale * scale * scale * by_scale * (1.0 / d))
        by_h = (dy[r, :].astype(F32) + by_wide.astype(BF16).astype(F32)).astype(BF16)
        dy[r, :] = by_h
        dyt[:, r] = by_h.T
        at[:, r] = a[0, r, :].T
        return 0

    lax.fori_loop(0, steps, norm_back, 0)

    def first_layer(c, _):
        def between_halves():
            @pl.when(c >= 1)
            def _():
                gu_round(2 * (chunks + c) - 1)

        backward(0, c, between_halves)
        gu_round(2 * (chunks + c))

        @pl.when(c + early < n)
        def _():
            dn_round(1, c + early)
        return 0

    lax.fori_loop(0, chunks, first_layer, 0)
    for t in range(chunks + early, n):
        dn_round(1, t)

    def drain(k, _):
        @pl.when(k < n - 1)
        def _():
            gu_round(2 * slabs - 1 + k)
        dn_round(0, k)
        return 0

    lax.fori_loop(0, n, drain, 0)

    outs = []
    for layer in range(2):
        for which, dst in enumerate((gg_hbm, gu_hbm)):
            src = dgu.at[layer, which, pl.ds(pl.multiple_of(me * rows, 16), rows), :]
            outs.append(pltpu.make_async_copy(src, dst.at[layer], out_sem.at[len(outs)]))
        src = dd.at[layer, pl.ds(pl.multiple_of(me * down, 16), down), :]
        outs.append(pltpu.make_async_copy(src, gd_hbm.at[layer], out_sem.at[len(outs)]))
    for one in outs:
        one.start()
    sums = jnp.zeros((1, 1), F32)
    for layer in range(2):
        for which in range(2):
            v = dgu[layer, which, pl.ds(pl.multiple_of(me * rows, 16), rows), :].astype(F32)
            sums += jnp.sum(v * v, keepdims=True)
        v = dd[layer, pl.ds(pl.multiple_of(me * down, 16), down), :].astype(F32)
        sums += jnp.sum(v * v, keepdims=True)
    mine[...] = jnp.broadcast_to(sums, mine.shape)

    def spread(k):
        return pltpu.make_async_remote_copy(mine, squares.at[k - 1], sq_send.at[k - 1], sq_recv.at[k - 1],
                                            device_id={"dp": lax.rem(me + k, n)}, device_id_type=MESH)

    for k in range(1, n):
        spread(k).start()
    for k in range(1, n):
        spread(k).wait_recv()
    total = mine[...]
    for k in range(1, n):
        total += squares[k - 1]
    total_ref[...] = total
    for k in range(1, n):
        spread(k).wait_send()
    for one in outs:
        one.wait()


def summed_gradients(n, x, dy, w_gate, w_up, w_down):
    _, tokens, d = x.shape
    layers, rows, ff = w_gate.shape
    down = w_down.shape[1]
    dims = (tokens, d, ff, rows, down)
    half = down // 2
    dma = pltpu.SemaphoreType.DMA
    anywhere = pl.BlockSpec(memory_space=pl.ANY)
    return pl.pallas_call(
        functools.partial(kernel, n, dims),
        out_shape=(
            jax.ShapeDtypeStruct(w_gate.shape, BF16),
            jax.ShapeDtypeStruct(w_up.shape, BF16),
            jax.ShapeDtypeStruct(w_down.shape, BF16),
            jax.ShapeDtypeStruct((8, 128), F32),
        ),
        in_specs=[anywhere] * 5,
        out_specs=(anywhere,) * 3 + (pl.BlockSpec(memory_space=pltpu.VMEM),),
        scratch_shapes=[
            pltpu.VMEM((layers, 2, d, ff), BF16),
            pltpu.VMEM((layers, ff, d), BF16),
            pltpu.VMEM((layers, 2, d, ff), BF16),
            pltpu.VMEM((layers, ff, d), BF16),
            pltpu.VMEM((tokens, d), BF16),
            pltpu.VMEM((tokens, d), BF16),
            pltpu.VMEM((layers, tokens, d), BF16),
            pltpu.VMEM((d, tokens), BF16),
            pltpu.VMEM((d, tokens), BF16),
            pltpu.VMEM((tokens, d), F32),
            pltpu.VMEM((tokens, CHUNK), BF16),
            pltpu.VMEM((tokens, 2 * CHUNK), BF16),
            pltpu.VMEM((2, 2, n - 1, rows, CHUNK), BF16),
            pltpu.VMEM((2, 2, 2, d // 128, half, 128), BF16),
            pltpu.VMEM((n - 1, 8, 128), F32),
            pltpu.VMEM((8, 128), F32),
            dma((8,)),
            dma((6,)),
            dma((2, 3, 2, 2)),
            dma((2, 3, 2, 2)),
            dma((2, 3, 2, 2)),
            dma((2, 3, 2, 2)),
            dma((2, 2, n - 1)),
            dma((2, 2, n - 1)),
            dma((2, 2, 2, d // 128)),
            dma((2, 2, d // 128)),
            dma((n - 1,)),
            dma((n - 1,)),
        ],
        compiler_params=pltpu.CompilerParams(collective_id=0, has_side_effects=True, vmem_limit_bytes=67_000_000),
    )(x, dy, w_gate, w_up, w_down)


def adamw(w, m, v, g):
    m = 0.9 * m + 0.1 * g
    v = 0.95 * v + 0.05 * g * g
    step = m * lax.rsqrt(v + 1e-8) + 0.1 * w
    return (w - 0.02 * step).astype(BF16), m, v


def solution(mesh):
    n = mesh.shape["dp"]

    def step(x, dy, *arrays):
        weights, m, v = (arrays[i : i + 3] for i in (0, 3, 6))
        *gradients, squares = summed_gradients(n, x, dy, *weights)
        count = n * sum(g.size for g in gradients)
        factor = jnp.minimum(1.0, 0.5 * lax.rsqrt(squares[0, 0] / count + 1e-30))
        new = [adamw(w.astype(F32), m, v, g.astype(F32) * factor) for w, m, v, g in zip(weights, m, v, gradients, strict=True)]
        return tuple(one[which] for which in range(3) for one in new)

    states, cut = P(("rep", "dp"), None, None), P(None, "dp", None)
    return jax.shard_map(
        step,
        mesh=mesh,
        in_specs=(states, states) + (cut,) * 9,
        out_specs=(P("rep", "dp", None),) * 9,
        check_vma=False,
    )
```

```python
import functools

import jax
import jax.numpy as jnp
from jax import lax
from jax.experimental import pallas as pl
from jax.experimental.pallas import tpu as pltpu
from jax.sharding import PartitionSpec as P

F32, BF16 = jnp.float32, jnp.bfloat16
MESH = pl.DeviceIdType.MESH
CHUNK = 256
TILE = 512
SMALL = 256


def dot(a, b):
    return jnp.dot(a, b, preferred_element_type=F32)


def dot_t(a, b):
    return lax.dot_general(a, b, (((1,), (1,)), ((), ())), preferred_element_type=F32)


def scale_of(wide):
    return lax.rsqrt(jnp.mean(wide * wide, -1, keepdims=True) + 1e-6)


def kernel(n, dims, x_hbm, dy_hbm, wg_hbm, wu_hbm, wd_hbm, gg_hbm, gu_hbm, gd_hbm, total_ref,
           wgu, wd, dgu, dd, h, dy, a, at, dyt, acc, hid, dgdu, gu_slot, dn_slot, squares, mine,
           load_sem, out_sem, zrecv, zsend, drecv, dsend, yrecv, ysend, erecv, esend, gu_recv, gu_send, dn_recv, dn_send, sq_recv, sq_send):
    tokens, d, ff, rows, down = dims
    half = down // 2
    chunks = ff // CHUNK
    me = lax.axis_index("dp")
    rep = lax.axis_index("rep")
    core = lax.rem(rep, 2)
    partner = rep + 1 - 2 * core
    side = lax.rem(rep // 2, 2)
    beside = rep + 2 - 4 * side
    ahead = (lax.rem(me + 1, n), lax.rem(me + n - 1, n))

    def to(direction):
        return {"dp": ahead[direction]}

    loads = []
    for layer in range(2):
        for which, src in enumerate((wg_hbm, wu_hbm)):
            dst = wgu.at[layer, which, pl.ds(pl.multiple_of(me * rows, 16), rows), :]
            loads.append(pltpu.make_async_copy(src.at[layer], dst, load_sem.at[len(loads)]))
        dst = wd.at[layer, pl.ds(pl.multiple_of(me * down, 16), down), :]
        loads.append(pltpu.make_async_copy(wd_hbm.at[layer], dst, load_sem.at[len(loads)]))
    loads.append(pltpu.make_async_copy(x_hbm.at[0], h, load_sem.at[6]))
    loads.append(pltpu.make_async_copy(dy_hbm.at[0], dy, load_sem.at[7]))
    for one in loads:
        one.start()
    barrier = pltpu.get_barrier_semaphore()
    for k in range(1, n):
        pl.semaphore_signal(barrier, inc=1, device_id={"dp": lax.rem(me + k, n)}, device_id_type=MESH)
    pl.semaphore_signal(barrier, inc=1, device_id={"rep": partner}, device_id_type=MESH)
    pl.semaphore_signal(barrier, inc=1, device_id={"rep": beside}, device_id_type=MESH)
    pl.semaphore_wait(barrier, n + 1)
    for one in loads[:6]:
        one.wait()

    lanes = ff // 128
    ahead_cut = (lanes // 2 + 1) // 2 * 128
    gu_size = (ahead_cut, ff // 2 - ahead_cut)
    dn_size = (half // 16 // 2 * 16, half - half // 16 // 2 * 16)
    dn_cut = (d // 128 + 1) // 2 * 128
    pieces = 4

    def piece(layer, matrix, which, number, direction, block):
        if number < 2:
            size = gu_size[direction]
            cut = (size // 128 + 1) // 2 * 128
            off, size_ = (0, cut) if number == 0 else (cut, size - cut)
            start = (2 * gu_size[0] if direction else 0) + which * size + off
            r = pl.ds(pl.multiple_of(block * rows, 16), rows)
            return wgu.at[layer, matrix, r, pl.ds(pl.multiple_of(start, 128), size_)]
        start = block * down + which * half + (dn_size[0] if direction else 0)
        lane = pl.ds(0, dn_cut) if number == 2 else pl.ds(dn_cut, d - dn_cut)
        return wd.at[layer, pl.ds(pl.multiple_of(start, 16), dn_size[direction]), lane]

    def held(direction, t):
        return lax.rem(me - t + n, n) if direction == 0 else lax.rem(me + t, n)

    def send(ref, out_sem, in_sem, layer, number, direction, t, device):
        slot = lax.rem(t, 2)
        return pltpu.make_async_remote_copy(ref, ref, out_sem.at[layer, number, direction, slot], in_sem.at[layer, number, direction, slot],
                                            device_id=device, device_id_type=MESH)

    def along(layer, number, direction, t):
        ref = piece(layer, side, core, number, direction, held(direction, t))
        return send(ref, zsend, zrecv, layer, number, direction, t, to(direction))

    def arrived(layer, number, direction, t):
        ref = piece(layer, side, core, number, direction, held(direction, t))
        return send(ref, zsend, zrecv, layer, number, direction, t - 1, to(direction))

    def across(layer, which, number, direction, t):
        ref = piece(layer, side, which, number, direction, held(direction, t))
        return send(ref, dsend, drecv, layer, number, direction, t, {"rep": partner})

    def over(layer, matrix, number, direction, t):
        ref = piece(layer, matrix, core, number, direction, held(direction, t))
        return send(ref, ysend, yrecv, layer, number, direction, t, {"rep": beside})

    def onward(layer, which, number, direction, t):
        ref = piece(layer, 1 - side, which, number, direction, held(direction, t))
        return send(ref, esend, erecv, layer, number, direction, t, {"rep": partner})

    def when(condition, f):
        pl.when(condition)(f)

    def gather_round(layer, t):
        for number in range(pieces):
            for direction in range(2):
                when((t >= 1) & (t < n), lambda: arrived(layer, number, direction, t).wait_recv())
                when((t >= 2) & (t <= n), lambda: across(layer, 1 - core, number, direction, t - 1).wait_recv())
            for direction in range(2):
                when((t >= 2) & (t <= n), lambda: along(layer, number, direction, t - 2).wait_send())
                when(t <= n - 2, lambda: along(layer, number, direction, t).start())
                when(t >= 3, lambda: across(layer, core, number, direction, t - 2).wait_send())
                when((t >= 1) & (t < n), lambda: across(layer, core, number, direction, t).start())
        for number in range(2):
            for direction in range(2):
                when((t >= 2) & (t <= n), lambda: over(layer, 1 - side, number, direction, t - 1).wait_recv())
                when(t >= 3, lambda: onward(layer, 1 - core, number, direction, t - 2).wait_recv())
            for direction in range(2):
                when(t >= 3, lambda: over(layer, side, number, direction, t - 2).wait_send())
                when((t >= 1) & (t < n), lambda: over(layer, side, number, direction, t).start())
                when(t >= 4, lambda: onward(layer, core, number, direction, t - 3).wait_send())
                when((t >= 2) & (t <= n), lambda: onward(layer, core, number, direction, t - 1).start())

    def gather_end(layer):
        for number in range(2):
            for direction in range(2):
                onward(layer, core, number, direction, n - 1).wait_send()

    def small(k):
        return pl.ds(pl.multiple_of(k * SMALL, SMALL), SMALL)

    steps = tokens // SMALL

    gather_round(0, 0)
    for one in loads[6:]:
        one.wait()

    def first(t, _):
        @pl.when(t >= 1)
        def _():
            gather_round(0, t)

        @pl.when(t < steps)
        def _():
            wide = h[small(t), :].astype(F32)
            a[0, small(t), :] = (wide * scale_of(wide)).astype(BF16)
            dyt[:, small(t)] = dy[small(t), :].T
            acc[small(t), :] = jnp.zeros((SMALL, d), F32)
        return 0

    lax.fori_loop(0, max(n + 2, steps), first, 0)
    gather_end(0)

    def cols(c):
        return pl.ds(pl.multiple_of(c * CHUNK, CHUNK), CHUNK)

    def forward(c, _):
        gather_round(1, c)

        def tile(k, _):
            r = pl.ds(pl.multiple_of(k * TILE, TILE), TILE)
            both = dot(a[0, r, :], jnp.concatenate([wgu[0, 0, :, cols(c)], wgu[0, 1, :, cols(c)]], 1))
            gate, up = both[:, :CHUNK], both[:, CHUNK:]
            hidden = (gate * jax.nn.sigmoid(gate) * up).astype(BF16)
            acc[r, :] += dot(hidden, wd[0, cols(c), :])
            return 0

        lax.fori_loop(0, tokens // TILE, tile, 0)
        return 0

    lax.fori_loop(0, chunks, forward, 0)
    for t in range(chunks, n):
        gather_round(1, t)

    def between(k, _):
        r = small(k)
        h1 = (h[r, :].astype(F32) + acc[r, :].astype(BF16).astype(F32)).astype(BF16)
        h[r, :] = h1
        wide = h1.astype(F32)
        a1 = (wide * scale_of(wide)).astype(BF16)
        a[1, r, :] = a1
        at[:, r] = a1.T
        acc[r, :] = jnp.zeros((SMALL, d), F32)
        return 0

    lax.fori_loop(0, steps, between, 0)
    for t in (n, n + 1):
        gather_round(1, t)
    gather_end(1)

    slabs = 2 * chunks

    def block_at(direction, t):
        return lax.rem(me - 1 - t + 2 * n, n) if direction == 0 else lax.rem(me + 1 + t, n)

    def gu_ref(j, direction, t):
        layer = 1 - j // chunks
        r = pl.ds(pl.multiple_of(block_at(direction, t) * rows, 16), rows)
        return dgu.at[layer, direction, r, cols(lax.rem(j, chunks))]

    def gu_copy(j, direction, t):
        slot = lax.rem(j, 2)
        return pltpu.make_async_remote_copy(gu_ref(j, direction, t), gu_slot.at[direction, slot, t], gu_send.at[direction, slot, t],
                                            gu_recv.at[direction, slot, t], device_id=to(direction), device_id_type=MESH)

    def gu_round(r):
        def tick(k, _):
            i = n // 2 - 1 - k
            t = lax.rem(r, 2) + 2 * i
            j = r // 2 - i

            @pl.when((j >= 0) & (j < slabs))
            def _():
                @pl.when(t >= 1)
                def _():
                    for direction in range(2):
                        gu_copy(j, direction, t - 1).wait_recv()
                        mine_ref = gu_ref(j, direction, t)
                        got = gu_slot[direction, lax.rem(j, 2), t - 1].astype(F32)
                        mine_ref[...] = (got + mine_ref[...].astype(F32)).astype(BF16)
                    for direction in range(2):
                        gu_copy(j, direction, t - 1).wait_send()

                @pl.when(t <= n - 2)
                def _():
                    for direction in range(2):
                        gu_copy(j, direction, t).start()
            return 0

        lax.fori_loop(0, n // 2, tick, 0)

    parts = d // 128

    def dn_ref(layer, s, direction, t):
        r = pl.ds(pl.multiple_of(block_at(direction, t) * down + direction * half, 16), half)
        return dd.at[layer, r, pl.ds(pl.multiple_of(s * 128, 128), 128)]

    def dn_copy(layer, s, direction, t):
        slot = lax.rem(t, 2)
        return pltpu.make_async_remote_copy(dn_ref(layer, s, direction, t), dn_slot.at[layer, direction, slot, s], dn_send.at[layer, direction, s],
                                            dn_recv.at[layer, direction, slot, s], device_id=to(direction), device_id_type=MESH)

    def dn_round(layer, t):
        def part(s, _):
            @pl.when(t >= 1)
            def _():
                for direction in range(2):
                    dn_copy(layer, s, direction, t - 1).wait_recv()
                    mine_ref = dn_ref(layer, s, direction, t)
                    got = dn_slot[layer, direction, lax.rem(t + 1, 2), s].astype(F32)
                    mine_ref[...] = (got + mine_ref[...].astype(F32)).astype(BF16)
                for direction in range(2):
                    dn_copy(layer, s, direction, t - 1).wait_send()

            @pl.when(t <= n - 2)
            def _():
                for direction in range(2):
                    dn_copy(layer, s, direction, t).start()
            return 0

        lax.fori_loop(0, parts, part, 0)

    def backward(layer, c, between_halves):
        def tile(k, _):
            pl.when(k == tokens // TILE - 1)(between_halves)
            r = pl.ds(pl.multiple_of(k * TILE, TILE), TILE)
            wide = jnp.concatenate([wgu[layer, 0, :, cols(c)], wgu[layer, 1, :, cols(c)]], 1)
            both = dot(a[layer, r, :], wide)
            gate, up = both[:, :CHUNK], both[:, CHUNK:]
            by = dot_t(dy[r, :], wd[layer, cols(c), :]).astype(BF16).astype(F32)
            sig = jax.nn.sigmoid(gate)
            silu = gate * sig
            hid[r, :] = (silu * up).astype(BF16)
            by_gate = (by * up * (sig + silu * (1.0 - sig))).astype(BF16)
            by_up = (by * silu).astype(BF16)
            by_both = jnp.concatenate([by_gate, by_up], 1)
            dgdu[r, :] = by_both
            if layer == 1:
                acc[r, :] += dot_t(by_both, wide)
            return 0

        lax.fori_loop(0, tokens // TILE, tile, 0)
        by_w = dot(at[...], dgdu[...])
        dgu[layer, 0, :, cols(c)] = by_w[:, :CHUNK].astype(BF16)
        dgu[layer, 1, :, cols(c)] = by_w[:, CHUNK:].astype(BF16)
        dd[layer, cols(c), :] = dot(dyt[...], hid[...]).T.astype(BF16)

    def last_layer(c, _):
        def between_halves():
            @pl.when(c >= 1)
            def _():
                gu_round(2 * c - 1)

        backward(1, c, between_halves)
        gu_round(2 * c)
        return 0

    lax.fori_loop(0, chunks, last_layer, 0)

    early = min(2, steps)

    def norm_back(k, _):
        r = small(k)

        @pl.when(k == 0)
        def _():
            dn_round(1, 0)

        @pl.when(k == steps // 2)
        def _():
            gu_round(2 * chunks - 1)
            dn_round(1, 1)
        by_a = acc[r, :].astype(BF16).astype(F32)
        wide = h[r, :].astype(F32)
        scale = scale_of(wide)
        by_scale = jnp.sum(by_a * wide, -1, keepdims=True)
        by_wide = by_a * scale - wide * (scale * scale * scale * by_scale * (1.0 / d))
        by_h = (dy[r, :].astype(F32) + by_wide.astype(BF16).astype(F32)).astype(BF16)
        dy[r, :] = by_h
        dyt[:, r] = by_h.T
        at[:, r] = a[0, r, :].T
        return 0

    lax.fori_loop(0, steps, norm_back, 0)

    def first_layer(c, _):
        def between_halves():
            @pl.when(c >= 1)
            def _():
                gu_round(2 * (chunks + c) - 1)

        backward(0, c, between_halves)
        gu_round(2 * (chunks + c))

        @pl.when(c + early < n)
        def _():
            dn_round(1, c + early)
        return 0

    lax.fori_loop(0, chunks, first_layer, 0)
    for t in range(chunks + early, n):
        dn_round(1, t)

    def drain(k, _):
        @pl.when(k < n - 1)
        def _():
            gu_round(2 * slabs - 1 + k)
        dn_round(0, k)
        return 0

    lax.fori_loop(0, n, drain, 0)

    outs = []
    for layer in range(2):
        for which, dst in enumerate((gg_hbm, gu_hbm)):
            src = dgu.at[layer, which, pl.ds(pl.multiple_of(me * rows, 16), rows), :]
            outs.append(pltpu.make_async_copy(src, dst.at[layer], out_sem.at[len(outs)]))
        src = dd.at[layer, pl.ds(pl.multiple_of(me * down, 16), down), :]
        outs.append(pltpu.make_async_copy(src, gd_hbm.at[layer], out_sem.at[len(outs)]))
    for one in outs:
        one.start()
    sums = jnp.zeros((1, 1), F32)
    for layer in range(2):
        for which in range(2):
            v = dgu[layer, which, pl.ds(pl.multiple_of(me * rows, 16), rows), :].astype(F32)
            sums += jnp.sum(v * v, keepdims=True)
        v = dd[layer, pl.ds(pl.multiple_of(me * down, 16), down), :].astype(F32)
        sums += jnp.sum(v * v, keepdims=True)
    mine[...] = jnp.broadcast_to(sums, mine.shape)

    def spread(k):
        return pltpu.make_async_remote_copy(mine, squares.at[k - 1], sq_send.at[k - 1], sq_recv.at[k - 1],
                                            device_id={"dp": lax.rem(me + k, n)}, device_id_type=MESH)

    for k in range(1, n):
        spread(k).start()
    for k in range(1, n):
        spread(k).wait_recv()
    total = mine[...]
    for k in range(1, n):
        total += squares[k - 1]
    total_ref[...] = total
    for k in range(1, n):
        spread(k).wait_send()
    for one in outs:
        one.wait()


def summed_gradients(n, x, dy, w_gate, w_up, w_down):
    _, tokens, d = x.shape
    layers, rows, ff = w_gate.shape
    down = w_down.shape[1]
    dims = (tokens, d, ff, rows, down)
    half = down // 2
    dma = pltpu.SemaphoreType.DMA
    anywhere = pl.BlockSpec(memory_space=pl.ANY)
    return pl.pallas_call(
        functools.partial(kernel, n, dims),
        out_shape=(
            jax.ShapeDtypeStruct(w_gate.shape, BF16),
            jax.ShapeDtypeStruct(w_up.shape, BF16),
            jax.ShapeDtypeStruct(w_down.shape, BF16),
            jax.ShapeDtypeStruct((8, 128), F32),
        ),
        in_specs=[anywhere] * 5,
        out_specs=(anywhere,) * 3 + (pl.BlockSpec(memory_space=pltpu.VMEM),),
        scratch_shapes=[
            pltpu.VMEM((layers, 2, d, ff), BF16),
            pltpu.VMEM((layers, ff, d), BF16),
            pltpu.VMEM((layers, 2, d, ff), BF16),
            pltpu.VMEM((layers, ff, d), BF16),
            pltpu.VMEM((tokens, d), BF16),
            pltpu.VMEM((tokens, d), BF16),
            pltpu.VMEM((layers, tokens, d), BF16),
            pltpu.VMEM((d, tokens), BF16),
            pltpu.VMEM((d, tokens), BF16),
            pltpu.VMEM((tokens, d), F32),
            pltpu.VMEM((tokens, CHUNK), BF16),
            pltpu.VMEM((tokens, 2 * CHUNK), BF16),
            pltpu.VMEM((2, 2, n - 1, rows, CHUNK), BF16),
            pltpu.VMEM((2, 2, 2, d // 128, half, 128), BF16),
            pltpu.VMEM((n - 1, 8, 128), F32),
            pltpu.VMEM((8, 128), F32),
            dma((8,)),
            dma((6,)),
            dma((2, 4, 2, 2)),
            dma((2, 4, 2, 2)),
            dma((2, 4, 2, 2)),
            dma((2, 4, 2, 2)),
            dma((2, 2, 2, 2)),
            dma((2, 2, 2, 2)),
            dma((2, 2, 2, 2)),
            dma((2, 2, 2, 2)),
            dma((2, 2, n - 1)),
            dma((2, 2, n - 1)),
            dma((2, 2, 2, d // 128)),
            dma((2, 2, d // 128)),
            dma((n - 1,)),
            dma((n - 1,)),
        ],
        compiler_params=pltpu.CompilerParams(collective_id=0, has_side_effects=True, vmem_limit_bytes=67_000_000),
    )(x, dy, w_gate, w_up, w_down)


def adamw(w, m, v, g):
    m = 0.9 * m + 0.1 * g
    v = 0.95 * v + 0.05 * g * g
    step = m * lax.rsqrt(v + 1e-8) + 0.1 * w
    return (w - 0.02 * step).astype(BF16), m, v


def solution(mesh):
    n = mesh.shape["dp"]

    def step(x, dy, *arrays):
        weights, m, v = (arrays[i : i + 3] for i in (0, 3, 6))
        *gradients, squares = summed_gradients(n, x, dy, *weights)
        count = n * sum(g.size for g in gradients)
        factor = jnp.minimum(1.0, 0.5 * lax.rsqrt(squares[0, 0] / count + 1e-30))
        new = [adamw(w.astype(F32), m, v, g.astype(F32) * factor) for w, m, v, g in zip(weights, m, v, gradients, strict=True)]
        return tuple(one[which] for which in range(3) for one in new)

    states, cut = P(("rep", "dp"), None, None), P(None, "dp", None)
    return jax.shard_map(
        step,
        mesh=mesh,
        in_specs=(states, states) + (cut,) * 9,
        out_specs=(P("rep", "dp", None),) * 9,
        check_vma=False,
    )
```
